8 devices in a mesh: part: 1 (over z), loc: 2 (over y), grp: 4 (over x, core).
Axes of the slice: x: 2, y: 2, z: 1, core: 2. Of those that a mesh axis runs over, the one named last changes fastest.
Arguments:
- x_tok: bfloat16 [2048, 2048], P(('part', 'grp', 'loc'))
- expert_ids: int32 [2048, 8], P(('part', 'grp', 'loc'))
- gate_val: float32 [2048, 8], P(('part', 'grp', 'loc'))
- w_gate: bfloat16 [64, 2048, 1024], P(('grp', 'loc'))
- w_up: bfloat16 [64, 2048, 1024], P(('grp', 'loc'))
- w_down: bfloat16 [64, 1024, 2048], P(('grp', 'loc'))
Outputs:
- output: bfloat16 [2048, 2048], P(('part', 'grp', 'loc'))
All inputs are finite; a program needn't handle non-finite values.
Results may differ from the reference program's by a relative error of at most 0.0123254.
Values are sent between devices in bfloat16 or wider.
A program may use at most 1 GiB of HBM per device.

```python
import jax
import jax.numpy as jnp
from jax import lax

D = 2048
FF = 1024
EXPERTS = 64
TOP = 8
MAXG = 4
TOK_DEV = 256
GROUPS = 4
LOCS = 2

TOKENS = TOK_DEV * GROUPS * LOCS
PER_GROUP = EXPERTS // GROUPS
HIT_GROUPS = min(MAXG, GROUPS)
PER_HIT = TOP // HIT_GROUPS
CAP = 8 * (TOKENS * TOP // (4 * EXPERTS) + 1)
HOT_TOKENS = min(TOKENS, CAP * PER_GROUP // PER_HIT)


def draw_routing(route_key):
    key_grp, key_tok, key_exp = jax.random.split(route_key, 3)
    grp_order = jax.random.permutation(key_grp, GROUPS)
    tok_rank = jnp.arange(TOKENS)
    has_hot = tok_rank < HOT_TOKENS
    seq_base = jnp.where(has_hot, tok_rank * (HIT_GROUPS - 1), HOT_TOKENS * (HIT_GROUPS - 1) + (tok_rank - HOT_TOKENS) * HIT_GROUPS)
    choice = jnp.arange(HIT_GROUPS)
    other_pos = seq_base[:, None] + choice[None, :] - has_hot[:, None].astype(jnp.int32)
    other_grp = grp_order[1 + other_pos % (GROUPS - 1)]
    chosen = jnp.where(has_hot[:, None] & (choice[None, :] == 0), grp_order[0], other_grp)
    member = jnp.sum((chosen[:, :, None] == jnp.arange(GROUPS)[None, None, :]).astype(jnp.int32), axis=1)
    before = jnp.cumsum(member, axis=0) - member
    order_in = jnp.take_along_axis(before, chosen, axis=1)[:, :, None]
    pick_ids = jnp.arange(PER_HIT)[None, None, :]
    is_hot = (chosen == grp_order[0])[:, :, None]
    hot_seq = jnp.where(order_in < CAP, order_in * (PER_HIT - 1) + pick_ids - 1, CAP * (PER_HIT - 1) + (order_in - CAP) * PER_HIT + pick_ids)
    hot_slot = jnp.where((order_in < CAP) & (pick_ids == 0), 0, 1 + hot_seq % (PER_GROUP - 1))
    cold_slot = (order_in * PER_HIT + pick_ids) % PER_GROUP
    slot_pos = jnp.where(is_hot, hot_slot, cold_slot)
    grp_perm = jax.vmap(lambda sub_key: jax.random.permutation(sub_key, PER_GROUP))(jax.random.split(key_exp, GROUPS))
    local_ids = grp_perm[chosen[:, :, None], slot_pos]
    experts = (chosen[:, :, None] * PER_GROUP + local_ids).reshape(TOKENS, TOP)
    shuffle = jax.random.permutation(key_tok, TOKENS)
    return experts[shuffle].astype(jnp.int32)


def setup_inputs(seed: int = 0, part: int = 0) -> dict:
    root_key = jax.random.key(seed)
    key_part = jax.random.fold_in(root_key, part)
    key_x, key_route, key_gate = jax.random.split(key_part, 3)
    key_one, key_two, key_three = jax.random.split(jax.random.key(seed + 7919), 3)
    x_tok = jax.random.normal(key_x, (TOKENS, D), jnp.float32).astype(jnp.bfloat16)
    expert_ids = draw_routing(key_route)
    gate_val = jax.random.uniform(key_gate, (TOKENS, TOP), jnp.float32, 0.5, 1.5) * TOP ** -0.5
    w_gate = (jax.random.normal(key_one, (EXPERTS, D, FF), jnp.float32) * D ** -0.5).astype(jnp.bfloat16)
    w_up = (jax.random.normal(key_two, (EXPERTS, D, FF), jnp.float32) * D ** -0.5).astype(jnp.bfloat16)
    w_down = (jax.random.normal(key_three, (EXPERTS, FF, D), jnp.float32) * FF ** -0.5).astype(jnp.bfloat16)
    return {"x_tok": x_tok, "expert_ids": expert_ids, "gate_val": gate_val, "w_gate": w_gate, "w_up": w_up, "w_down": w_down}


def reference(x_tok, expert_ids, gate_val, w_gate, w_up, w_down):
    n_slots = TOKENS * TOP
    flat_ids = expert_ids.reshape(-1)
    sort_order = jnp.argsort(flat_ids, stable=True)
    sorted_ids = flat_ids[sort_order]
    counts = jnp.bincount(flat_ids, length=EXPERTS)
    starts = jnp.cumsum(counts) - counts
    slot_ids = sorted_ids * CAP + jnp.arange(n_slots) - starts[sorted_ids]
    src_tok = jnp.zeros(EXPERTS * CAP, jnp.int32).at[slot_ids].set((sort_order // TOP).astype(jnp.int32))
    src_gate = jnp.zeros(EXPERTS * CAP, jnp.float32).at[slot_ids].set(gate_val.reshape(-1)[sort_order])
    stacked = (src_tok.reshape(GROUPS, PER_GROUP, CAP), src_gate.reshape(GROUPS, PER_GROUP, CAP), w_gate.reshape(GROUPS, PER_GROUP, D, FF), w_up.reshape(GROUPS, PER_GROUP, D, FF), w_down.reshape(GROUPS, PER_GROUP, FF, D))

    def expert_step(group_acc, expert_in):
        tok_rows, row_gate, w_one, w_two, w_three = expert_in
        picked_rows = x_tok[tok_rows]
        up_gate = jnp.dot(picked_rows, w_one, preferred_element_type=jnp.float32)
        up_lin = jnp.dot(picked_rows, w_two, preferred_element_type=jnp.float32)
        hidden = (jax.nn.silu(up_gate) * up_lin).astype(jnp.bfloat16)
        out_rows = jnp.dot(hidden, w_three, preferred_element_type=jnp.float32)
        return group_acc.at[tok_rows].add(out_rows * row_gate[:, None]), None

    def group_step(y_acc, group_in):
        zero_acc = jnp.zeros((TOKENS, D), jnp.float32)
        group_sum = lax.scan(expert_step, zero_acc, group_in)[0]
        return y_acc + group_sum.astype(jnp.bfloat16).astype(jnp.float32), None

    y_sum = lax.scan(group_step, jnp.zeros((TOKENS, D), jnp.float32), stacked)[0]
    return y_sum.astype(jnp.bfloat16)
```

```python
import functools

import jax
import jax.numpy as jnp
from jax import lax
from jax.experimental import pallas as pl
from jax.experimental.pallas import tpu as pltpu
from jax.sharding import PartitionSpec as P

MESH = pl.DeviceIdType.MESH
LANES = 128
ROW_BLOCK = 272
STRIDE = 280
TILE = 256


def share_kernel(n_grp, n_loc, mine_ref, all_ref, send_sem, recv_sem):
    grp, loc = lax.axis_index("grp"), lax.axis_index("loc")
    n_dev = n_grp * n_loc

    def peer(r):
        return {"grp": grp ^ (r % n_grp), "loc": loc ^ (r // n_grp)}

    barrier = pltpu.get_barrier_semaphore()
    for r in range(1, n_dev):
        pl.semaphore_signal(barrier, inc=1, device_id=peer(r), device_id_type=MESH)
    pl.semaphore_wait(barrier, n_dev - 1)
    copies = []
    for r in range(1, n_dev):
        copy = pltpu.make_async_remote_copy(
            src_ref=mine_ref, dst_ref=all_ref.at[r], send_sem=send_sem.at[r], recv_sem=recv_sem.at[r], device_id=peer(r), device_id_type=MESH
        )
        copy.start()
        copies.append(copy)
    all_ref[0] = mine_ref[...]
    for copy in copies:
        copy.wait()


def zero_acc(acc):
    def zero(i, c):
        acc[pl.ds(i * 16, 16)] = jnp.zeros((16,) + acc.shape[1:], jnp.float32)
        return c

    lax.fori_loop(0, acc.shape[0] // 16, zero, 0)


def down_scatter(e, base, rows, n_tok, list_ref, gate_ref, hid, wd_ref, ot, acc):
    half = wd_ref.shape[2]
    chunks = half // LANES

    def down(q, c):
        cols = pl.ds(pl.multiple_of(q * TILE, TILE), TILE)
        o = jnp.dot(hid, wd_ref[0, :, cols], preferred_element_type=jnp.float32)
        for k in range(TILE // LANES):
            start = pl.multiple_of((q * (TILE // LANES) + k) * STRIDE, 8)
            ot[pl.ds(start, ROW_BLOCK), :] = o[:, k * LANES:(k + 1) * LANES]
        return c

    lax.fori_loop(0, half // TILE, down, 0)

    def scatter(i, c):
        slots, sums = [], []
        for k in range(8):
            m = i * 8 + k
            t = list_ref[e, base + m]
            s = jnp.where(m < rows, t, n_tok + k)
            slots.append(s)
            sums.append(acc[s] + gate_ref[e, t] * ot[pl.ds(m, chunks, stride=STRIDE), :])
        for s, v in zip(slots, sums):
            acc[s] = v
        return c

    lax.fori_loop(0, (rows + 7) // 8, scatter, 0)


def write_out(acc, keep_ref, send_refs, sem):
    n_keep = keep_ref.shape[0]
    block = n_keep // len(send_refs)
    copies = [pltpu.make_async_copy(acc.at[pl.ds(n_keep + k * block, block)], ref, sem.at[k]) for k, ref in enumerate(send_refs)]
    copies.append(pltpu.make_async_copy(acc.at[pl.ds(0, n_keep)], keep_ref, sem.at[len(send_refs)]))
    for copy in copies:
        copy.start()
    for copy in copies:
        copy.wait()


def first_kernel(n_local, chunks, n_tok, x_places, n_x, cnt_ref, list_ref, gate_ref, *refs):
    x_hbm, (wg_ref, wu_ref, wd_ref, hid_ref, keep_ref), refs = refs[:n_x], refs[n_x:n_x + 5], refs[n_x + 5:]
    send_refs, (x_ref, acc, xs, xg, in_sem, out_sem) = refs[:-6], refs[-6:]
    e = pl.program_id(0)
    d_ff = wg_ref.shape[2]

    @pl.when(e == 0)
    def _():
        copies = [pltpu.make_async_copy(src, x_ref.at[pl.ds(at, src.shape[0])], in_sem.at[k]) for k, (src, at) in enumerate(zip(x_hbm, x_places))]
        for copy in copies:
            copy.start()
        zero_acc(acc)
        for copy in copies:
            copy.wait()

    n = cnt_ref[e]

    def block(b, carry):
        base = b * ROW_BLOCK
        rows = jnp.minimum(ROW_BLOCK, n - base)

        def gather(i, c):
            for k in range(8):
                m = i * 8 + k
                row = x_ref[list_ref[e, base + m]]
                xs[pl.ds(m, chunks, stride=STRIDE), :] = row.astype(jnp.float32)
            return c

        lax.fori_loop(0, (rows + 7) // 8, gather, 0)
        for j in range(chunks):
            xg[:, j * LANES:(j + 1) * LANES] = xs[pl.ds(j * STRIDE, ROW_BLOCK), :].astype(jnp.bfloat16)
        here = pl.ds(pl.multiple_of(base, 16), ROW_BLOCK)

        def up(q, c):
            cols = pl.ds(pl.multiple_of(q * TILE, TILE), TILE)
            u = jnp.dot(xg[...], wg_ref[0, :, cols], preferred_element_type=jnp.float32)
            v = jnp.dot(xg[...], wu_ref[0, :, cols], preferred_element_type=jnp.float32)
            hid_ref[0, here, cols] = (jax.nn.silu(u) * v).astype(jnp.bfloat16)
            return c

        lax.fori_loop(0, d_ff // TILE, up, 0)
        down_scatter(e, base, rows, n_tok, list_ref, gate_ref, hid_ref[0, here, :], wd_ref, xs, acc)
        return carry

    lax.fori_loop(0, (n + ROW_BLOCK - 1) // ROW_BLOCK, block, 0)

    @pl.when(e == n_local - 1)
    def _():
        write_out(acc, keep_ref, send_refs, out_sem)


def second_kernel(n_local, n_tok, cnt_ref, list_ref, gate_ref, hid_ref, wd_ref, keep_ref, *refs):
    send_refs, (acc, ot, out_sem) = refs[:-3], refs[-3:]
    e = pl.program_id(0)

    @pl.when(e == 0)
    def _():
        zero_acc(acc)

    n = cnt_ref[e]

    def block(b, carry):
        base = b * ROW_BLOCK
        rows = jnp.minimum(ROW_BLOCK, n - base)
        here = pl.ds(pl.multiple_of(base, 16), ROW_BLOCK)
        down_scatter(e, base, rows, n_tok, list_ref, gate_ref, hid_ref[0, here, :], wd_ref, ot, acc)
        return carry

    lax.fori_loop(0, (n + ROW_BLOCK - 1) // ROW_BLOCK, block, 0)

    @pl.when(e == n_local - 1)
    def _():
        write_out(acc, keep_ref, send_refs, out_sem)


def solution(mesh):
    n_grp = mesh.shape["grp"]
    n_loc = mesh.shape["loc"]
    n_dev = n_grp * n_loc
    tok_spec = P(("part", "grp", "loc"), None)
    w_spec = P(("grp", "loc"), None, None)

    def swap_grp(a, bits):
        return lax.ppermute(a, "grp", [(i, i ^ bits) for i in range(n_grp)])

    def swap_loc(a):
        return lax.ppermute(a, "loc", [(i, i ^ 1) for i in range(n_loc)])

    def device_step(x_tok, expert_ids, gate_val, w_gate, w_up, w_down):
        tok_local, d_model = x_tok.shape
        d_ff = w_gate.shape[2]
        chunks = d_model // LANES
        n_local = w_gate.shape[0]
        per_group = n_local * n_loc
        n_tok = tok_local * n_dev
        top_k = expert_ids.shape[1]
        capacity = 8 * (n_tok * top_k // (4 * per_group * n_grp) + 1)
        list_len = -(-capacity // ROW_BLOCK) * ROW_BLOCK
        me = lax.axis_index("grp") * n_loc + lax.axis_index("loc")

        own = x_tok.reshape(tok_local, chunks, LANES)
        mid = tok_local // 2
        from_y = swap_loc(own)
        from_x = swap_grp(own, 2)
        from_c = swap_grp(own, 1)
        diag_lo = swap_loc(from_x[:mid])
        diag_hi = swap_grp(from_y[mid:], 2)
        x_parts = [own, from_c, from_x, swap_grp(from_x, 1), from_y, swap_grp(from_y, 1), diag_lo, diag_hi, swap_grp(diag_lo, 1), swap_grp(diag_hi, 1)]
        x_places = [0, 1, 2, 3, 4, 5, 6, 6.5, 7, 7.5]
        x_places = [int(p * tok_local) for p in x_places]

        meta = jnp.concatenate([expert_ids.astype(jnp.float32).T, gate_val.T], axis=0)
        meta_all = pl.pallas_call(
            functools.partial(share_kernel, n_grp, n_loc),
            out_shape=jax.ShapeDtypeStruct((n_dev,) + meta.shape, jnp.float32),
            in_specs=[pl.BlockSpec(memory_space=pltpu.VMEM)],
            out_specs=pl.BlockSpec(memory_space=pltpu.VMEM),
            scratch_shapes=[pltpu.SemaphoreType.DMA((n_dev,)), pltpu.SemaphoreType.DMA((n_dev,))],
            compiler_params=pltpu.CompilerParams(collective_id=0, has_side_effects=True),
            name="share",
        )(meta)
        meta_all = meta_all.transpose(1, 0, 2).reshape(2 * top_k, n_tok)
        ids = meta_all[:top_k].astype(jnp.int32)
        gates = meta_all[top_k:]
        match = ids[None] == jnp.arange(n_local)[:, None, None] + me * n_local
        hit = jnp.any(match, axis=1)
        gate_of = jnp.sum(jnp.where(match, gates[None], 0.0), axis=1)
        rank = jnp.cumsum(hit.astype(jnp.int32), axis=1)
        count = rank[:, -1]
        rows = jnp.sum((rank[:, None, :] <= jnp.arange(list_len)[None, :, None]).astype(jnp.int32), axis=2)
        rows = jnp.minimum(rows, n_tok - 1)

        half = d_model // 2
        half_chunks = half // LANES
        n_keep = n_tok // n_loc
        part = jax.ShapeDtypeStruct((tok_local, half_chunks, LANES), jnp.float32)
        keep = jax.ShapeDtypeStruct((n_keep, half_chunks, LANES), jnp.float32)
        any_spec = pl.BlockSpec(memory_space=pl.ANY)
        acc = pltpu.VMEM((n_tok + 16, half_chunks, LANES), jnp.float32)
        hid_spec = pl.BlockSpec((1, list_len, d_ff), lambda e, *_: (e, 0, 0))
        params = pltpu.CompilerParams(vmem_limit_bytes=62_000_000, dimension_semantics=("arbitrary",))
        first = pl.pallas_call(
            functools.partial(first_kernel, n_local, chunks, n_tok, x_places, len(x_parts)),
            grid_spec=pltpu.PrefetchScalarGridSpec(
                num_scalar_prefetch=3,
                grid=(n_local,),
                in_specs=[any_spec] * len(x_parts)
                + [
                    pl.BlockSpec((1, d_model, d_ff), lambda e, *_: (e, 0, 0)),
                    pl.BlockSpec((1, d_model, d_ff), lambda e, *_: (e, 0, 0)),
                    pl.BlockSpec((1, d_ff, half), lambda e, *_: (e, 0, 0)),
                ],
                out_specs=[hid_spec] + [any_spec] * (1 + n_grp),
                scratch_shapes=[
                    pltpu.VMEM((n_tok, chunks, LANES), jnp.bfloat16),
                    acc,
                    pltpu.VMEM((chunks * STRIDE, LANES), jnp.float32),
                    pltpu.VMEM((ROW_BLOCK, d_model), jnp.bfloat16),
                    pltpu.SemaphoreType.DMA((len(x_parts),)),
                    pltpu.SemaphoreType.DMA((1 + n_grp,)),
                ],
            ),
            out_shape=[jax.ShapeDtypeStruct((n_local, list_len, d_ff), jnp.bfloat16), keep] + [part] * n_grp,
            compiler_params=params,
            cost_estimate=pl.CostEstimate(flops=20 * 10**9, bytes_accessed=90 * 10**6, transcendentals=0),
            name="first",
        )
        hid, keep_a, *send_a = first(count, rows, gate_of, *x_parts, w_gate, w_up, w_down)
        second = pl.pallas_call(
            functools.partial(second_kernel, n_local, n_tok),
            grid_spec=pltpu.PrefetchScalarGridSpec(
                num_scalar_prefetch=3,
                grid=(n_local,),
                in_specs=[hid_spec, pl.BlockSpec((1, d_ff, half), lambda e, *_: (e, 0, 1))],
                out_specs=[any_spec] * (1 + n_grp),
                scratch_shapes=[acc, pltpu.VMEM((half_chunks * STRIDE, LANES), jnp.float32), pltpu.SemaphoreType.DMA((1 + n_grp,))],
            ),
            out_shape=[keep] + [part] * n_grp,
            compiler_params=params,
            cost_estimate=pl.CostEstimate(flops=4 * 10**9, bytes_accessed=30 * 10**6, transcendentals=0),
            name="second",
        )
        keep_b, *send_b = second(count, rows, gate_of, hid, w_down)

        def home(keep_rows, sends):
            total = None
            for k in (2, 3, 1, 0):
                mixed = (keep_rows[k * tok_local:(k + 1) * tok_local] + swap_loc(sends[k])).astype(jnp.bfloat16)
                back = swap_grp(mixed, k) if k else mixed
                back = back.astype(jnp.float32)
                total = back if total is None else total + back
            return total.astype(jnp.bfloat16).reshape(tok_local, half)

        return jnp.concatenate([home(keep_a, send_a), home(keep_b, send_b)], axis=1)

    return jax.shard_map(device_step, mesh=mesh, in_specs=(tok_spec, tok_spec, tok_spec, w_spec, w_spec, w_spec), out_specs=tok_spec, check_vma=False)
```

```python
import functools

import jax
import jax.numpy as jnp
from jax import lax
from jax.experimental import pallas as pl
from jax.experimental.pallas import tpu as pltpu
from jax.sharding import PartitionSpec as P

MESH = pl.DeviceIdType.MESH
LANES = 128
ROW_BLOCK = 272
STRIDE = 276
TILE = 256
PAD = 16
STEP = 16
SEND_ORDER = (2, 3, 1, 0)


def share_kernel(n_grp, n_loc, mine_ref, all_ref, send_sem, recv_sem):
    grp, loc = lax.axis_index("grp"), lax.axis_index("loc")
    n_dev = n_grp * n_loc

    def peer(r):
        return {"grp": grp ^ (r % n_grp), "loc": loc ^ (r // n_grp)}

    barrier = pltpu.get_barrier_semaphore()
    for r in range(1, n_dev):
        pl.semaphore_signal(barrier, inc=1, device_id=peer(r), device_id_type=MESH)
    pl.semaphore_wait(barrier, n_dev - 1)
    copies = []
    for r in range(1, n_dev):
        copy = pltpu.make_async_remote_copy(
            src_ref=mine_ref, dst_ref=all_ref.at[r], send_sem=send_sem.at[r], recv_sem=recv_sem.at[r], device_id=peer(r), device_id_type=MESH
        )
        copy.start()
        copies.append(copy)
    all_ref[0] = mine_ref[...]
    for copy in copies:
        copy.wait()


def zero_acc(acc):
    def zero(i, c):
        acc[pl.ds(i * 16, 16)] = jnp.zeros((16,) + acc.shape[1:], jnp.float32)
        return c

    lax.fori_loop(0, acc.shape[0] // 16, zero, 0)


def gather_rows(list_ref, at, first, count, x_ref, xs):
    chunks = x_ref.shape[1]
    for k in range(count):
        row = x_ref[list_ref[at + (first + k)]]
        xs[pl.ds(first + k, chunks, stride=STRIDE), :] = row.astype(jnp.float32)


def scatter_rows(list_ref, at, gate_ref, gate_at, first, count, ot, acc):
    chunks = acc.shape[1]
    for k0 in range(0, count, 4):
        slots, sums = [], []
        for k in range(k0, min(k0 + 4, count)):
            s = list_ref[at + (first + k)]
            slots.append(s)
            sums.append(acc[s] + gate_ref[gate_at + s] * ot[pl.ds(first + k, chunks, stride=STRIDE), :])
        for s, v in zip(slots, sums):
            acc[s] = v


def down_block(hid, wd_ref, ot):
    for q in range(wd_ref.shape[2] // TILE):
        o = jnp.dot(hid, wd_ref[0, :, q * TILE:(q + 1) * TILE], preferred_element_type=jnp.float32)
        for k in range(TILE // LANES):
            ot[pl.ds((q * (TILE // LANES) + k) * STRIDE, ROW_BLOCK), :] = o[:, k * LANES:(k + 1) * LANES]


def write_out(acc, keep_ref, send_refs, sem):
    n_keep = keep_ref.shape[0]
    block = n_keep // len(send_refs)
    copies = [pltpu.make_async_copy(acc.at[pl.ds(n_keep + k * block, block)], send_refs[k], sem.at[k]) for k in SEND_ORDER]
    copies.append(pltpu.make_async_copy(acc.at[pl.ds(0, n_keep)], keep_ref, sem.at[len(send_refs)]))
    for copy in copies:
        copy.start()
    for copy in copies:
        copy.wait()


def first_kernel(n_local, list_len, n_pad, x_places, n_x, cnt_ref, list_ref, gate_ref, *refs):
    x_hbm, (wg_ref, wu_ref, wd_ref, hid_ref, keep_ref), refs = refs[:n_x], refs[n_x:n_x + 5], refs[n_x + 5:]
    send_refs, (x_ref, acc, xs, ot, xg, in_sem, out_sem) = refs[:-7], refs[-7:]
    e = pl.program_id(0)
    d_ff = wg_ref.shape[2]

    @pl.when(e == 0)
    def _():
        copies = [pltpu.make_async_copy(src, x_ref.at[pl.ds(at, src.shape[0])], in_sem.at[k]) for k, (src, at) in enumerate(zip(x_hbm, x_places))]
        for copy in copies:
            copy.start()
        zero_acc(acc)
        for copy in copies:
            copy.wait()

    n = cnt_ref[e]

    def block(b, carry):
        base = b * ROW_BLOCK
        at = e * list_len + base
        here = pl.ds(pl.multiple_of(base, 16), ROW_BLOCK)
        steps = (jnp.minimum(ROW_BLOCK, n - base) + STEP - 1) // STEP

        def gather(q, c):
            gather_rows(list_ref, at, q * STEP, STEP, x_ref, xs)
            return c

        lax.fori_loop(0, steps, gather, 0)
        for j in range(x_ref.shape[1]):
            xg[:, j * LANES:(j + 1) * LANES] = xs[pl.ds(j * STRIDE, ROW_BLOCK), :].astype(jnp.bfloat16)

        def up(q, c):
            cols = pl.ds(pl.multiple_of(q * TILE, TILE), TILE)
            u = jnp.dot(xg[...], wg_ref[0, :, cols], preferred_element_type=jnp.float32)
            v = jnp.dot(xg[...], wu_ref[0, :, cols], preferred_element_type=jnp.float32)
            hid_ref[0, here, cols] = (jax.nn.silu(u) * v).astype(jnp.bfloat16)
            return c

        lax.fori_loop(0, d_ff // TILE, up, 0)
        down_block(hid_ref[0, here, :], wd_ref, ot)

        def scatter(q, c):
            scatter_rows(list_ref, at, gate_ref, e * n_pad, q * STEP, STEP, ot, acc)
            return c

        lax.fori_loop(0, steps, scatter, 0)
        return carry

    lax.fori_loop(0, (n + ROW_BLOCK - 1) // ROW_BLOCK, block, 0)

    @pl.when(e == n_local - 1)
    def _():
        write_out(acc, keep_ref, send_refs, out_sem)


def second_kernel(n_local, list_len, n_pad, cnt_ref, list_ref, gate_ref, hid_ref, wd_ref, keep_ref, *refs):
    send_refs, (acc, ot, out_sem) = refs[:-3], refs[-3:]
    e = pl.program_id(0)

    @pl.when(e == 0)
    def _():
        zero_acc(acc)

    n = cnt_ref[e]

    def block(b, carry):
        base = b * ROW_BLOCK
        here = pl.ds(pl.multiple_of(base, 16), ROW_BLOCK)
        down_block(hid_ref[0, here, :], wd_ref, ot)

        steps = (jnp.minimum(ROW_BLOCK, n - base) + STEP - 1) // STEP

        def scatter(q, c):
            scatter_rows(list_ref, e * list_len + base, gate_ref, e * n_pad, q * STEP, STEP, ot, acc)
            return c

        lax.fori_loop(0, steps, scatter, 0)
        return carry

    lax.fori_loop(0, (n + ROW_BLOCK - 1) // ROW_BLOCK, block, 0)

    @pl.when(e == n_local - 1)
    def _():
        write_out(acc, keep_ref, send_refs, out_sem)


def solution(mesh):
    n_grp = mesh.shape["grp"]
    n_loc = mesh.shape["loc"]
    n_dev = n_grp * n_loc
    tok_spec = P(("part", "grp", "loc"), None)
    w_spec = P(("grp", "loc"), None, None)

    def swap_grp(a, bits):
        return lax.ppermute(a, "grp", [(i, i ^ bits) for i in range(n_grp)])

    def swap_loc(a):
        return lax.ppermute(a, "loc", [(i, i ^ 1) for i in range(n_loc)])

    def device_step(x_tok, expert_ids, gate_val, w_gate, w_up, w_down):
        tok_local, d_model = x_tok.shape
        d_ff = w_gate.shape[2]
        chunks = d_model // LANES
        n_local = w_gate.shape[0]
        per_group = n_local * n_loc
        n_tok = tok_local * n_dev
        top_k = expert_ids.shape[1]
        capacity = 8 * (n_tok * top_k // (4 * per_group * n_grp) + 1)
        list_len = -(-capacity // ROW_BLOCK) * ROW_BLOCK
        me = lax.axis_index("grp") * n_loc + lax.axis_index("loc")

        meta = jnp.concatenate([expert_ids.astype(jnp.float32).T, gate_val.T], axis=0)
        meta_all = pl.pallas_call(
            functools.partial(share_kernel, n_grp, n_loc),
            out_shape=jax.ShapeDtypeStruct((n_dev,) + meta.shape, jnp.float32),
            in_specs=[pl.BlockSpec(memory_space=pltpu.VMEM)],
            out_specs=pl.BlockSpec(memory_space=pltpu.VMEM),
            scratch_shapes=[pltpu.SemaphoreType.DMA((n_dev,)), pltpu.SemaphoreType.DMA((n_dev,))],
            compiler_params=pltpu.CompilerParams(collective_id=0, has_side_effects=True),
            name="share",
        )(meta)
        own = x_tok.reshape(tok_local, chunks, LANES)
        own, meta_all = lax.optimization_barrier((own, meta_all))
        mid = tok_local // 2
        low, high = own[:mid], own[mid:]
        x_low, y_high = swap_grp(low, 2), swap_loc(high)
        x_high, y_low = swap_grp(high, 2), swap_loc(low)
        own_c = swap_grp(own, 1)
        d_low, d_high = swap_loc(x_low), swap_grp(y_high, 2)
        x_parts = [own, own_c, x_low, x_high, swap_grp(x_low, 1), swap_grp(x_high, 1), y_low, y_high, swap_grp(y_low, 1), swap_grp(y_high, 1), d_low, d_high, swap_grp(d_low, 1), swap_grp(d_high, 1)]
        x_places = [0, 2, 4, 5, 6, 7, 8, 9, 10, 11, 12, 13, 14, 15]
        x_places = [p * mid for p in x_places]

        meta_all = meta_all.transpose(1, 0, 2).reshape(2 * top_k, n_tok)
        ids = meta_all[:top_k].astype(jnp.int32)
        gates = meta_all[top_k:]
        match = ids[None] == jnp.arange(n_local)[:, None, None] + me * n_local
        hit = jnp.any(match, axis=1)
        gate_of = jnp.sum(jnp.where(match, gates[None], 0.0), axis=1)
        rank = jnp.cumsum(hit.astype(jnp.int32), axis=1)
        count = rank[:, -1]
        place = jnp.arange(list_len)[None, :]
        rows = jnp.sum((rank[:, None, :] <= place[:, :, None]).astype(jnp.int32), axis=2)
        rows = jnp.where(place < count[:, None], rows, n_tok + place % PAD)
        rows = rows.reshape(-1)
        n_pad = n_tok + PAD
        gate_of = jnp.pad(gate_of, ((0, 0), (0, PAD))).reshape(-1)

        half = d_model // 2
        half_chunks = half // LANES
        n_keep = n_tok // n_loc
        part = jax.ShapeDtypeStruct((tok_local, half_chunks, LANES), jnp.float32)
        keep = jax.ShapeDtypeStruct((n_keep, half_chunks, LANES), jnp.float32)
        any_spec = pl.BlockSpec(memory_space=pl.ANY)
        acc = pltpu.VMEM((n_pad, half_chunks, LANES), jnp.float32)
        hid_spec = pl.BlockSpec((1, list_len, d_ff), lambda e, *_: (e, 0, 0))
        params = pltpu.CompilerParams(vmem_limit_bytes=62_000_000, dimension_semantics=("arbitrary",))
        first = pl.pallas_call(
            functools.partial(first_kernel, n_local, list_len, n_pad, x_places, len(x_parts)),
            grid_spec=pltpu.PrefetchScalarGridSpec(
                num_scalar_prefetch=3,
                grid=(n_local,),
                in_specs=[any_spec] * len(x_parts)
                + [
                    pl.BlockSpec((1, d_model, d_ff), lambda e, *_: (e, 0, 0)),
                    pl.BlockSpec((1, d_model, d_ff), lambda e, *_: (e, 0, 0)),
                    pl.BlockSpec((1, d_ff, half), lambda e, *_: (e, 0, 0)),
                ],
                out_specs=[hid_spec] + [any_spec] * (1 + n_grp),
                scratch_shapes=[
                    pltpu.VMEM((n_pad, chunks, LANES), jnp.bfloat16),
                    acc,
                    pltpu.VMEM((chunks * STRIDE, LANES), jnp.float32),
                    pltpu.VMEM((half_chunks * STRIDE, LANES), jnp.float32),
                    pltpu.VMEM((ROW_BLOCK, d_model), jnp.bfloat16),
                    pltpu.SemaphoreType.DMA((len(x_parts),)),
                    pltpu.SemaphoreType.DMA((1 + n_grp,)),
                ],
            ),
            out_shape=[jax.ShapeDtypeStruct((n_local, list_len, d_ff), jnp.bfloat16), keep] + [part] * n_grp,
            compiler_params=params,
            cost_estimate=pl.CostEstimate(flops=20 * 10**9, bytes_accessed=90 * 10**6, transcendentals=0),
            name="first",
        )
        hid, keep_a, *send_a = first(count, rows, gate_of, *x_parts, w_gate, w_up, w_down)
        second = pl.pallas_call(
            functools.partial(second_kernel, n_local, list_len, n_pad),
            grid_spec=pltpu.PrefetchScalarGridSpec(
                num_scalar_prefetch=3,
                grid=(n_local,),
                in_specs=[hid_spec, pl.BlockSpec((1, d_ff, half), lambda e, *_: (e, 0, 1))],
                out_specs=[any_spec] * (1 + n_grp),
                scratch_shapes=[acc, pltpu.VMEM((half_chunks * STRIDE, LANES), jnp.float32), pltpu.SemaphoreType.DMA((1 + n_grp,))],
            ),
            out_shape=[keep] + [part] * n_grp,
            compiler_params=params,
            cost_estimate=pl.CostEstimate(flops=4 * 10**9, bytes_accessed=30 * 10**6, transcendentals=0),
            name="second",
        )
        keep_b, *send_b = second(count, rows, gate_of, hid, w_down)

        def home(keep_rows, sends):
            total = None
            for k in SEND_ORDER:
                mixed = (keep_rows[k * tok_local:(k + 1) * tok_local] + swap_loc(sends[k])).astype(jnp.bfloat16)
                back = swap_grp(mixed, k) if k else mixed
                back = back.astype(jnp.float32)
                total = back if total is None else total + back
            return total.astype(jnp.bfloat16).reshape(tok_local, half)

        return jnp.concatenate([home(keep_a, send_a), home(keep_b, send_b)], axis=1)

    return jax.shard_map(device_step, mesh=mesh, in_specs=(tok_spec, tok_spec, tok_spec, w_spec, w_spec, w_spec), out_specs=tok_spec, check_vma=False)
```

```python
import functools

import jax
import jax.numpy as jnp
from jax import lax
from jax.experimental import pallas as pl
from jax.experimental.pallas import tpu as pltpu
from jax.sharding import PartitionSpec as P


MESH = pl.DeviceIdType.MESH
LANES = 128
TILE = 256
PAD = 16
STEP = 16
SLOTS = 2


def share_kernel(n_grp, n_loc, mine_ref, all_ref, send_sem, recv_sem):
    grp, loc = lax.axis_index("grp"), lax.axis_index("loc")
    n_dev = n_grp * n_loc

    def peer(r):
        return {"grp": grp ^ (r % n_grp), "loc": loc ^ (r // n_grp)}

    barrier = pltpu.get_barrier_semaphore()
    for r in range(1, n_dev):
        pl.semaphore_signal(barrier, inc=1, device_id=peer(r), device_id_type=MESH)
    pl.semaphore_wait(barrier, n_dev - 1)
    copies = []
    for r in range(1, n_dev):
        copy = pltpu.make_async_remote_copy(
            src_ref=mine_ref, dst_ref=all_ref.at[r], send_sem=send_sem.at[r], recv_sem=recv_sem.at[r], device_id=peer(r), device_id_type=MESH
        )
        copy.start()
        copies.append(copy)
    all_ref[0] = mine_ref[...]
    for copy in copies:
        copy.wait()


def zero_acc(acc):
    def zero(i, c):
        acc[pl.ds(i * 16, 16)] = jnp.zeros((16,) + acc.shape[1:], jnp.float32)
        return c

    lax.fori_loop(0, acc.shape[0] // 16, zero, 0)


def gather_rows(list_ref, at, first, x_ref, xs, stride):
    chunks = x_ref.shape[1]
    for k in range(STEP):
        row = x_ref[list_ref[at + (first + k)]]
        xs[pl.ds(first + k, chunks, stride=stride), :] = row.astype(jnp.float32)


def scatter_rows(list_ref, at, gate_ref, gate_at, first, ot, acc, stride):
    chunks = acc.shape[1]
    for k0 in range(0, STEP, 4):
        slots, sums = [], []
        for k in range(k0, k0 + 4):
            s = list_ref[at + (first + k)]
            slots.append(s)
            sums.append(acc[s] + gate_ref[gate_at + s] * ot[pl.ds(first + k, chunks, stride=stride), :])
        for s, v in zip(slots, sums):
            acc[s] = v


def pass_kernel(n_local, list_len, n_pad, row_block, x_places, out_places, cnt_ref, list_ref, gate_ref, *refs):
    n_x, n_out = len(x_places), len(out_places)
    stride = row_block + 4
    x_hbm, (wg_hbm, wu_hbm, wd_hbm), refs = refs[:n_x], refs[n_x:n_x + 3], refs[n_x + 3:]
    outs, (x_ref, acc, xs, xg, hid, wg_ref, wu_ref, wd_ref, x_sem, w_sem, out_sem) = refs[:n_out], refs[n_out:]
    d_ff, d_model = wd_ref.shape[1:]

    def weights(e, slot):
        return [
            pltpu.make_async_copy(wg_hbm.at[e], wg_ref.at[slot], w_sem.at[slot, 0]),
            pltpu.make_async_copy(wu_hbm.at[e], wu_ref.at[slot], w_sem.at[slot, 1]),
            pltpu.make_async_copy(wd_hbm.at[e], wd_ref.at[slot], w_sem.at[slot, 2]),
        ]

    x_copies = [pltpu.make_async_copy(src, x_ref.at[pl.ds(at, src.shape[0])], x_sem.at[k]) for k, (src, at) in enumerate(zip(x_hbm, x_places))]
    for copy in x_copies:
        copy.start()
    for e in range(SLOTS):
        for copy in weights(e, e):
            copy.start()
    zero_acc(acc)
    for copy in x_copies:
        copy.wait()

    def expert(e, carry):
        slot = lax.rem(e, SLOTS)
        n = cnt_ref[e]
        now = weights(e, slot)
        now[0].wait()
        now[1].wait()
        now[2].wait()

        def block(b, c):
            base = b * row_block
            at = e * list_len + base
            steps = (jnp.minimum(row_block, n - base) + STEP - 1) // STEP

            def gather(q, c):
                gather_rows(list_ref, at, q * STEP, x_ref, xs, stride)
                return c

            lax.fori_loop(0, steps, gather, 0)
            for j in range(d_model // LANES):
                xg[:, j * LANES:(j + 1) * LANES] = xs[pl.ds(j * stride, row_block), :].astype(jnp.bfloat16)
            for q in range(d_ff // TILE):
                cols = slice(q * TILE, (q + 1) * TILE)
                u = jnp.dot(xg[...], wg_ref[slot, :, cols], preferred_element_type=jnp.float32)
                v = jnp.dot(xg[...], wu_ref[slot, :, cols], preferred_element_type=jnp.float32)
                hid[:, cols] = (jax.nn.silu(u) * v).astype(jnp.bfloat16)
            for q in range(d_model // TILE):
                o = jnp.dot(hid[...], wd_ref[slot, :, q * TILE:(q + 1) * TILE], preferred_element_type=jnp.float32)
                for k in range(TILE // LANES):
                    xs[pl.ds((q * (TILE // LANES) + k) * stride, row_block), :] = o[:, k * LANES:(k + 1) * LANES]

            def scatter(q, c):
                scatter_rows(list_ref, at, gate_ref, e * n_pad, q * STEP, xs, acc, stride)
                return c

            lax.fori_loop(0, steps, scatter, 0)
            return c

        lax.fori_loop(0, (n + row_block - 1) // row_block, block, 0)

        @pl.when(e + SLOTS < n_local)
        def _():
            for copy in weights(e + SLOTS, slot):
                copy.start()

        return carry

    lax.fori_loop(0, n_local, expert, 0)
    out_copies = [pltpu.make_async_copy(acc.at[pl.ds(at, ref.shape[0])], ref, out_sem.at[k]) for k, (ref, at) in enumerate(zip(outs, out_places))]
    for copy in out_copies:
        copy.start()
    for copy in out_copies:
        copy.wait()


def solution(mesh):
    n_grp = mesh.shape["grp"]
    n_loc = mesh.shape["loc"]
    n_dev = n_grp * n_loc
    tok_spec = P(("part", "grp", "loc"), None)
    w_spec = P(("grp", "loc"), None, None)

    def swap_grp(a, bits):
        return lax.ppermute(a, "grp", [(i, i ^ bits) for i in range(n_grp)])

    def swap_loc(a):
        return lax.ppermute(a, "loc", [(i, i ^ 1) for i in range(n_loc)])

    def swap_diag(a):
        pairs = [(l * n_grp + g, (l ^ 1) * n_grp + (g ^ 2)) for l in range(n_loc) for g in range(n_grp)]
        return lax.ppermute(a, ("loc", "grp"), pairs)

    def device_step(x_tok, expert_ids, gate_val, w_gate, w_up, w_down):
        tok_local, d_model = x_tok.shape
        d_ff = w_gate.shape[2]
        chunks = d_model // LANES
        n_local = w_gate.shape[0]
        per_group = n_local * n_loc
        n_tok = tok_local * n_dev
        top_k = expert_ids.shape[1]
        capacity = 8 * (n_tok * top_k // (4 * per_group * n_grp) + 1)
        me = lax.axis_index("grp") * n_loc + lax.axis_index("loc")

        meta = jnp.concatenate([expert_ids.astype(jnp.float32).T, gate_val.T], axis=0)
        meta_all = pl.pallas_call(
            functools.partial(share_kernel, n_grp, n_loc),
            out_shape=jax.ShapeDtypeStruct((n_dev,) + meta.shape, jnp.float32),
            in_specs=[pl.BlockSpec(memory_space=pltpu.VMEM)],
            out_specs=pl.BlockSpec(memory_space=pltpu.VMEM),
            scratch_shapes=[pltpu.SemaphoreType.DMA((n_dev,)), pltpu.SemaphoreType.DMA((n_dev,))],
            compiler_params=pltpu.CompilerParams(collective_id=0, has_side_effects=True),
            name="share",
        )(meta)
        mid = tok_local // 2
        low, high = (x_tok[h * mid:(h + 1) * mid].reshape(mid, chunks, LANES) for h in range(2))
        low, high, meta_all = lax.optimization_barrier((low, high, meta_all))

        y_low = swap_loc(low)
        c_low = swap_grp(low, 1)
        yc_low = swap_grp(y_low, 1)
        y_high = swap_loc(high)
        x_low = swap_grp(low, 2)
        x_high = swap_grp(high, 2)
        d_low = swap_loc(x_low)
        late, y_low = lax.optimization_barrier((high, y_low))
        d_high = swap_diag(late)
        parts = {
            0: [low, high],
            1: [c_low, swap_grp(high, 1)],
            2: [x_low, x_high],
            3: [swap_grp(x_low, 1), swap_grp(x_high, 1)],
            4: [y_low, y_high],
            5: [yc_low, swap_grp(y_high, 1)],
            6: [d_low, d_high],
            7: [swap_grp(d_low, 1), swap_grp(d_high, 1)],
        }

        cube = meta_all.transpose(1, 0, 2).reshape(2 * top_k, 2, 2, 2, 2, mid)
        near_meta = cube[:, :, 0, :, 0].reshape(2 * top_k, -1)
        far_meta = jnp.concatenate([cube[:, :, 1].reshape(2 * top_k, 2, 4, mid), cube[:, :, 0, :, 1]], axis=2).reshape(2 * top_k, -1)
        any_spec = pl.BlockSpec(memory_space=pl.ANY)
        piece = jax.ShapeDtypeStruct((mid, chunks, LANES), jnp.float32)

        def run_pass(homes, meta, row_block, before=None):
            blocks = [(k + dy * n_grp, h) for dy in range(n_loc) for k, h in homes]
            n_rows = len(blocks) * mid
            n_pad = n_rows + PAD
            list_len = -(-min(capacity, n_rows) // row_block) * row_block
            ids = meta[:top_k].astype(jnp.int32)
            gates = meta[top_k:]
            match = ids[None] == jnp.arange(n_local)[:, None, None] + me * n_local
            hit = jnp.any(match, axis=1)
            gate_of = jnp.sum(jnp.where(match, gates[None], 0.0), axis=1)
            gate_of = jnp.pad(gate_of, ((0, 0), (0, PAD))).reshape(-1)
            rank = jnp.cumsum(hit.astype(jnp.int32), axis=1)
            count = rank[:, -1]
            place = jnp.arange(list_len)[None, :]
            rows = jnp.sum((rank[:, None, :] <= place[:, :, None]).astype(jnp.int32), axis=2)
            rows = jnp.where(place < count[:, None], rows, n_rows + place % PAD).reshape(-1)

            x_parts = [parts[r][h] for r, h in blocks]
            x_places = [p * mid for p in range(len(blocks))]
            out_places = x_places[len(homes):] + x_places[:len(homes)]
            stride = row_block + 4
            if before is not None:
                count, before = lax.optimization_barrier((count, before))
            run = pl.pallas_call(
                functools.partial(pass_kernel, n_local, list_len, n_pad, row_block, x_places, out_places),
                grid_spec=pltpu.PrefetchScalarGridSpec(
                    num_scalar_prefetch=3,
                    grid=(),
                    in_specs=[any_spec] * (len(x_parts) + 3),
                    out_specs=[any_spec] * len(out_places),
                    scratch_shapes=[
                        pltpu.VMEM((n_pad, chunks, LANES), jnp.bfloat16),
                        pltpu.VMEM((n_pad, chunks, LANES), jnp.float32),
                        pltpu.VMEM((chunks * stride, LANES), jnp.float32),
                        pltpu.VMEM((row_block, d_model), jnp.bfloat16),
                        pltpu.VMEM((row_block, d_ff), jnp.bfloat16),
                        pltpu.VMEM((SLOTS, d_model, d_ff), jnp.bfloat16),
                        pltpu.VMEM((SLOTS, d_model, d_ff), jnp.bfloat16),
                        pltpu.VMEM((SLOTS, d_ff, d_model), jnp.bfloat16),
                        pltpu.SemaphoreType.DMA((len(x_parts),)),
                        pltpu.SemaphoreType.DMA((SLOTS, 3)),
                        pltpu.SemaphoreType.DMA((len(out_places),)),
                    ],
                ),
                out_shape=[piece] * len(out_places),
                compiler_params=pltpu.CompilerParams(vmem_limit_bytes=62_000_000),
                cost_estimate=pl.CostEstimate(flops=25 * 10**9, bytes_accessed=110 * 10**6, transcendentals=0),
            )
            outs = run(count, rows, gate_of, *x_parts, w_gate, w_up, w_down)
            pieces = {home: (outs[i], outs[len(homes) + i]) for i, home in enumerate(homes)}
            return {**(before or {}), **pieces}

        near, far = [(0, 0), (1, 0)], [(2, 0), (2, 1), (3, 0), (3, 1), (0, 1), (1, 1)]
        pieces = run_pass(near, near_meta, 96)
        pieces = run_pass(far, far_meta, 208, pieces)

        totals = [None, None]
        for k, h in near + [(2, 0), (2, 1), (3, 0), (3, 1), (1, 1), (0, 1)]:
            send, keep = pieces[k, h]
            mixed = (keep + swap_loc(send)).astype(jnp.bfloat16)
            back = (swap_grp(mixed, k) if k else mixed).astype(jnp.float32)
            totals[h] = back if totals[h] is None else totals[h] + back
        y = jnp.concatenate(totals, axis=0).astype(jnp.bfloat16)
        return y.reshape(tok_local, d_model)

    return jax.shard_map(device_step, mesh=mesh, in_specs=(tok_spec, tok_spec, tok_spec, w_spec, w_spec, w_spec), out_specs=tok_spec, check_vma=False)
```

```python
import functools

import jax
import jax.numpy as jnp
from jax import lax
from jax.experimental import pallas as pl
from jax.experimental.pallas import tpu as pltpu
from jax.sharding import PartitionSpec as P


MESH = pl.DeviceIdType.MESH
LANES = 128
TILE = 256
PAD = 16
STEP = 16


def share_kernel(n_grp, n_loc, mine_ref, all_ref, send_sem, recv_sem):
    grp, loc = lax.axis_index("grp"), lax.axis_index("loc")
    n_dev = n_grp * n_loc

    def peer(r):
        return {"grp": grp ^ (r % n_grp), "loc": loc ^ (r // n_grp)}

    barrier = pltpu.get_barrier_semaphore()
    for r in range(1, n_dev):
        pl.semaphore_signal(barrier, inc=1, device_id=peer(r), device_id_type=MESH)
    pl.semaphore_wait(barrier, n_dev - 1)
    copies = []
    for r in range(1, n_dev):
        copy = pltpu.make_async_remote_copy(
            src_ref=mine_ref, dst_ref=all_ref.at[r], send_sem=send_sem.at[r], recv_sem=recv_sem.at[r], device_id=peer(r), device_id_type=MESH
        )
        copy.start()
        copies.append(copy)
    all_ref[0] = mine_ref[...]
    for copy in copies:
        copy.wait()


def zero_acc(acc):
    def zero(i, c):
        acc[pl.ds(i * 16, 16)] = jnp.zeros((16,) + acc.shape[1:], jnp.float32)
        return c

    lax.fori_loop(0, acc.shape[0] // 16, zero, 0)


def gather_rows(list_ref, at, first, x_ref, xs, stride):
    chunks = x_ref.shape[1]
    for k in range(STEP):
        row = x_ref[list_ref[at + (first + k)]]
        xs[pl.ds(first + k, chunks, stride=stride), :] = row.astype(jnp.float32)


def scatter_rows(list_ref, at, gate_ref, gate_at, first, ot, acc, stride):
    chunks = acc.shape[1]
    for k0 in range(0, STEP, 4):
        slots, sums = [], []
        for k in range(k0, k0 + 4):
            s = list_ref[at + (first + k)]
            slots.append(s)
            sums.append(acc[s] + gate_ref[gate_at + s] * ot[pl.ds(first + k, chunks, stride=stride), :])
        for s, v in zip(slots, sums):
            acc[s] = v


def pass_kernel(n_slots, split, n_local, list_len, n_pad, row_block, x_places, out_places, cnt_ref, list_ref, gate_ref, *refs):
    n_x, n_out = len(x_places), len(out_places)
    stride = row_block + 4
    x_hbm, (wg_hbm, wu_hbm, wd_hbm), refs = refs[:n_x], refs[n_x:n_x + 3], refs[n_x + 3:]
    outs, (x_ref, acc, xs, xg, hid, wg_ref, wu_ref, wd_ref, x_sem, w_sem, out_sem) = refs[:n_out], refs[n_out:]
    d_ff, d_model = wd_ref.shape[1:]

    def weights(e, slot):
        return [
            pltpu.make_async_copy(wg_hbm.at[e], wg_ref.at[slot], w_sem.at[slot, 0]),
            pltpu.make_async_copy(wu_hbm.at[e], wu_ref.at[slot], w_sem.at[slot, 1]),
            pltpu.make_async_copy(wd_hbm.at[e], wd_ref.at[slot], w_sem.at[slot, 2]),
        ]

    x_copies = [pltpu.make_async_copy(src, x_ref.at[pl.ds(at, src.shape[0])], x_sem.at[k]) for k, (src, at) in enumerate(zip(x_hbm, x_places))]
    for copy in x_copies:
        copy.start()
    for e in range(n_slots):
        for copy in weights(e, e):
            copy.start()
    zero_acc(acc)
    for copy in x_copies:
        copy.wait()

    def expert(e, carry):
        slot = lax.rem(e, n_slots)
        n = cnt_ref[e]
        now = weights(e, slot)
        ahead = weights(e + n_slots, slot)
        n_blocks = jnp.maximum((n + row_block - 1) // row_block, 1)
        if not split:
            for copy in now:
                copy.wait()

        def block(b, c):
            base = b * row_block
            at = e * list_len + base
            steps = (jnp.minimum(row_block, n - base) + STEP - 1) // STEP

            def gather(q, c):
                gather_rows(list_ref, at, q * STEP, x_ref, xs, stride)
                return c

            lax.fori_loop(0, steps, gather, 0)
            for j in range(d_model // LANES):
                xg[:, j * LANES:(j + 1) * LANES] = xs[pl.ds(j * stride, row_block), :].astype(jnp.bfloat16)

            if split:
                @pl.when(b == 0)
                def _():
                    now[0].wait()
                    now[1].wait()

            for q in range(d_ff // TILE):
                cols = slice(q * TILE, (q + 1) * TILE)
                u = jnp.dot(xg[...], wg_ref[slot, :, cols], preferred_element_type=jnp.float32)
                v = jnp.dot(xg[...], wu_ref[slot, :, cols], preferred_element_type=jnp.float32)
                hid[:, cols] = (jax.nn.silu(u) * v).astype(jnp.bfloat16)

            if split:
                @pl.when(b == 0)
                def _():
                    now[2].wait()

                @pl.when((b == n_blocks - 1) & (e + n_slots < n_local))
                def _():
                    ahead[0].start()
                    ahead[1].start()

            for q in range(d_model // TILE):
                o = jnp.dot(hid[...], wd_ref[slot, :, q * TILE:(q + 1) * TILE], preferred_element_type=jnp.float32)
                for k in range(TILE // LANES):
                    xs[pl.ds((q * (TILE // LANES) + k) * stride, row_block), :] = o[:, k * LANES:(k + 1) * LANES]

            def scatter(q, c):
                scatter_rows(list_ref, at, gate_ref, e * n_pad, q * STEP, xs, acc, stride)
                return c

            lax.fori_loop(0, steps, scatter, 0)
            return c

        lax.fori_loop(0, n_blocks, block, 0)

        @pl.when(e + n_slots < n_local)
        def _():
            for copy in ahead[2:] if split else ahead:
                copy.start()

        return carry

    lax.fori_loop(0, n_local, expert, 0)
    out_copies = [pltpu.make_async_copy(acc.at[pl.ds(at, ref.shape[0])], ref, out_sem.at[k]) for k, (ref, at) in enumerate(zip(outs, out_places))]
    for copy in out_copies:
        copy.start()
    for copy in out_copies:
        copy.wait()


def solution(mesh):
    n_grp = mesh.shape["grp"]
    n_loc = mesh.shape["loc"]
    n_dev = n_grp * n_loc
    tok_spec = P(("part", "grp", "loc"), None)
    w_spec = P(("grp", "loc"), None, None)

    def swap_grp(a, bits):
        return lax.ppermute(a, "grp", [(i, i ^ bits) for i in range(n_grp)])

    def swap_loc(a):
        return lax.ppermute(a, "loc", [(i, i ^ 1) for i in range(n_loc)])

    def swap_diag(a):
        pairs = [(l * n_grp + g, (l ^ 1) * n_grp + (g ^ 2)) for l in range(n_loc) for g in range(n_grp)]
        return lax.ppermute(a, ("loc", "grp"), pairs)

    def device_step(x_tok, expert_ids, gate_val, w_gate, w_up, w_down):
        tok_local, d_model = x_tok.shape
        d_ff = w_gate.shape[2]
        chunks = d_model // LANES
        n_local = w_gate.shape[0]
        per_group = n_local * n_loc
        n_tok = tok_local * n_dev
        top_k = expert_ids.shape[1]
        capacity = 8 * (n_tok * top_k // (4 * per_group * n_grp) + 1)
        me = lax.axis_index("grp") * n_loc + lax.axis_index("loc")

        meta = jnp.concatenate([expert_ids.astype(jnp.float32).T, gate_val.T], axis=0)
        meta_all = pl.pallas_call(
            functools.partial(share_kernel, n_grp, n_loc),
            out_shape=jax.ShapeDtypeStruct((n_dev,) + meta.shape, jnp.float32),
            in_specs=[pl.BlockSpec(memory_space=pltpu.VMEM)],
            out_specs=pl.BlockSpec(memory_space=pltpu.VMEM),
            scratch_shapes=[pltpu.SemaphoreType.DMA((n_dev,)), pltpu.SemaphoreType.DMA((n_dev,))],
            compiler_params=pltpu.CompilerParams(collective_id=0, has_side_effects=True),
            name="share",
        )(meta)
        mid = tok_local // 2
        low, high = (x_tok[h * mid:(h + 1) * mid].reshape(mid, chunks, LANES) for h in range(2))
        low, high, meta_all = lax.optimization_barrier((low, high, meta_all))

        y_low = swap_loc(low)
        c_low = swap_grp(low, 1)
        yc_low = swap_grp(y_low, 1)
        c_high = swap_grp(high, 1)
        y_high = swap_loc(high)
        x_low = swap_grp(low, 2)
        x_high = swap_grp(high, 2)
        d_low = swap_loc(x_low)
        late, y_low = lax.optimization_barrier((high, y_low))
        d_high = swap_diag(late)
        parts = {
            0: [low, high],
            1: [c_low, c_high],
            2: [x_low, x_high],
            3: [swap_grp(x_low, 1), swap_grp(x_high, 1)],
            4: [y_low, y_high],
            5: [yc_low, swap_grp(y_high, 1)],
            6: [d_low, d_high],
            7: [swap_grp(d_low, 1), swap_grp(d_high, 1)],
        }

        cube = meta_all.transpose(1, 0, 2).reshape(2 * top_k, 2, 2, 2, 2, mid)
        near_keep, near_send = [(0, 0), (0, 1), (1, 0), (1, 1), (2, 0), (3, 0)], [(4, 0), (5, 0)]
        far_keep, far_send = [(2, 1), (3, 1)], [(4, 1), (5, 1), (6, 0), (6, 1), (7, 0), (7, 1)]

        def join(*blocks):
            return jnp.concatenate([b.reshape(2 * top_k, -1, mid) for b in blocks], axis=1).reshape(2 * top_k, -1)

        any_spec = pl.BlockSpec(memory_space=pl.ANY)
        piece = jax.ShapeDtypeStruct((mid, chunks, LANES), jnp.float32)

        def run_pass(blocks, meta, row_block, n_slots, split, before=None):
            n_rows = len(blocks) * mid
            n_pad = n_rows + PAD
            list_len = -(-min(capacity, n_rows) // row_block) * row_block
            ids = meta[:top_k].astype(jnp.int32)
            gates = meta[top_k:]
            match = ids[None] == jnp.arange(n_local)[:, None, None] + me * n_local
            hit = jnp.any(match, axis=1)
            gate_of = jnp.sum(jnp.where(match, gates[None], 0.0), axis=1)
            gate_of = jnp.pad(gate_of, ((0, 0), (0, PAD))).reshape(-1)
            rank = jnp.cumsum(hit.astype(jnp.int32), axis=1)
            count = rank[:, -1]
            place = jnp.arange(list_len)[None, :]
            rows = jnp.sum((rank[:, None, :] <= place[:, :, None]).astype(jnp.int32), axis=2)
            rows = jnp.where(place < count[:, None], rows, n_rows + place % PAD).reshape(-1)

            x_parts = [parts[r][h] for r, h in blocks]
            x_places = [p * mid for p in range(len(blocks))]
            out_places = x_places
            stride = row_block + 4
            if before is not None:
                count, before = lax.optimization_barrier((count, before))
            run = pl.pallas_call(
                functools.partial(pass_kernel, n_slots, split, n_local, list_len, n_pad, row_block, x_places, out_places),
                grid_spec=pltpu.PrefetchScalarGridSpec(
                    num_scalar_prefetch=3,
                    grid=(),
                    in_specs=[any_spec] * (len(x_parts) + 3),
                    out_specs=[any_spec] * len(out_places),
                    scratch_shapes=[
                        pltpu.VMEM((n_pad, chunks, LANES), jnp.bfloat16),
                        pltpu.VMEM((n_pad, chunks, LANES), jnp.float32),
                        pltpu.VMEM((chunks * stride, LANES), jnp.float32),
                        pltpu.VMEM((row_block, d_model), jnp.bfloat16),
                        pltpu.VMEM((row_block, d_ff), jnp.bfloat16),
                        pltpu.VMEM((n_slots, d_model, d_ff), jnp.bfloat16),
                        pltpu.VMEM((n_slots, d_model, d_ff), jnp.bfloat16),
                        pltpu.VMEM((n_slots, d_ff, d_model), jnp.bfloat16),
                        pltpu.SemaphoreType.DMA((len(x_parts),)),
                        pltpu.SemaphoreType.DMA((n_slots, 3)),
                        pltpu.SemaphoreType.DMA((len(out_places),)),
                    ],
                ),
                out_shape=[piece] * len(out_places),
                compiler_params=pltpu.CompilerParams(vmem_limit_bytes=62_000_000),
                cost_estimate=pl.CostEstimate(flops=25 * 10**9, bytes_accessed=110 * 10**6, transcendentals=0),
            )
            outs = run(count, rows, gate_of, *x_parts, w_gate, w_up, w_down)
            return {**(before or {}), **dict(zip(blocks, outs))}

        pieces = run_pass(near_send + near_keep, join(cube[:, 1, 0, :, 0], cube[:, 0, 0], cube[:, 0, 1, :, 0]), 144, 3, True)
        pieces = run_pass(far_send + far_keep, join(cube[:, 1, 0, :, 1], cube[:, 1, 1], cube[:, 0, 1, :, 1]), 144, 3, True, pieces)

        totals = [None, None]
        for k, h in [(0, 0), (1, 0), (2, 0), (2, 1), (3, 0), (3, 1), (1, 1), (0, 1)]:
            send, keep = pieces[k + n_grp, h], pieces[k, h]
            mixed = (keep + swap_loc(send)).astype(jnp.bfloat16)
            back = (swap_grp(mixed, k) if k else mixed).astype(jnp.float32)
            totals[h] = back if totals[h] is None else totals[h] + back
        y = jnp.concatenate(totals, axis=0).astype(jnp.bfloat16)
        return y.reshape(tok_local, d_model)

    return jax.shard_map(device_step, mesh=mesh, in_specs=(tok_spec, tok_spec, tok_spec, w_spec, w_spec, w_spec), out_specs=tok_spec, check_vma=False)
```

```python
import functools

import jax
import jax.numpy as jnp
from jax import lax
from jax.experimental import pallas as pl
from jax.experimental.pallas import tpu as pltpu
from jax.sharding import PartitionSpec as P


MESH = pl.DeviceIdType.MESH
LANES = 128
TILE = 256
PAD = 16
STEP = 16
SLOTS = 3


def share_kernel(n_grp, n_loc, mine_ref, all_ref, send_sem, recv_sem):
    grp, loc = lax.axis_index("grp"), lax.axis_index("loc")
    n_dev = n_grp * n_loc

    def peer(r):
        return {"grp": grp ^ (r % n_grp), "loc": loc ^ (r // n_grp)}

    barrier = pltpu.get_barrier_semaphore()
    for r in range(1, n_dev):
        pl.semaphore_signal(barrier, inc=1, device_id=peer(r), device_id_type=MESH)
    pl.semaphore_wait(barrier, n_dev - 1)
    copies = []
    for r in range(1, n_dev):
        copy = pltpu.make_async_remote_copy(
            src_ref=mine_ref, dst_ref=all_ref.at[r], send_sem=send_sem.at[r], recv_sem=recv_sem.at[r], device_id=peer(r), device_id_type=MESH
        )
        copy.start()
        copies.append(copy)
    all_ref[0] = mine_ref[...]
    for copy in copies:
        copy.wait()


def zero_acc(acc):
    def zero(i, c):
        acc[pl.ds(i * 16, 16)] = jnp.zeros((16,) + acc.shape[1:], jnp.float32)
        return c

    lax.fori_loop(0, acc.shape[0] // 16, zero, 0)


def gather_rows(list_ref, at, first, x_ref, xs, stride):
    chunks = x_ref.shape[1]
    for k in range(STEP):
        row = x_ref[list_ref[at + (first + k)]]
        xs[pl.ds(first + k, chunks, stride=stride), :] = row.astype(jnp.float32)


def scatter_rows(list_ref, at, gate_ref, gate_at, first, ot, acc, stride):
    chunks = acc.shape[1]
    for k0 in range(0, STEP, 4):
        slots, sums = [], []
        for k in range(k0, k0 + 4):
            s = list_ref[at + (first + k)]
            slots.append(s)
            sums.append(acc[s] + gate_ref[gate_at + s] * ot[pl.ds(first + k, chunks, stride=stride), :])
        for s, v in zip(slots, sums):
            acc[s] = v


def pass_kernel(n_slots, n_local, list_len, n_pad, row_block, x_places, out_places, cnt_ref, list_ref, gate_ref, *refs):
    n_x, n_out = len(x_places), len(out_places)
    stride = row_block + 4
    x_hbm, (wg_hbm, wu_hbm, wd_hbm), refs = refs[:n_x], refs[n_x:n_x + 3], refs[n_x + 3:]
    outs, (x_ref, acc, xs, xg, hid, wg_ref, wu_ref, wd_ref, x_sem, w_sem, out_sem) = refs[:n_out], refs[n_out:]
    d_ff, d_model = wd_ref.shape[1:]

    def weights(e, slot):
        return [
            pltpu.make_async_copy(wg_hbm.at[e], wg_ref.at[slot], w_sem.at[slot, 0]),
            pltpu.make_async_copy(wu_hbm.at[e], wu_ref.at[slot], w_sem.at[slot, 1]),
            pltpu.make_async_copy(wd_hbm.at[e], wd_ref.at[slot], w_sem.at[slot, 2]),
        ]

    x_copies = [pltpu.make_async_copy(src, x_ref.at[pl.ds(at, src.shape[0])], x_sem.at[k]) for k, (src, at) in enumerate(zip(x_hbm, x_places))]
    for copy in x_copies:
        copy.start()
    for e in range(n_slots):
        for copy in weights(e, e):
            copy.start()
    zero_acc(acc)
    for copy in x_copies:
        copy.wait()

    def expert(e, carry):
        slot = lax.rem(e, n_slots)
        n = cnt_ref[e]
        now = weights(e, slot)
        ahead = weights(e + n_slots, slot)
        n_blocks = jnp.maximum((n + row_block - 1) // row_block, 1)

        def block(b, c):
            base = b * row_block
            at = e * list_len + base
            steps = (jnp.minimum(row_block, n - base) + STEP - 1) // STEP

            def gather(q, c):
                gather_rows(list_ref, at, q * STEP, x_ref, xs, stride)
                return c

            lax.fori_loop(0, steps, gather, 0)
            for j in range(d_model // LANES):
                xg[:, j * LANES:(j + 1) * LANES] = xs[pl.ds(j * stride, row_block), :].astype(jnp.bfloat16)

            @pl.when(b == 0)
            def _():
                now[0].wait()
                now[1].wait()

            for q in range(d_ff // TILE):
                cols = slice(q * TILE, (q + 1) * TILE)
                u = jnp.dot(xg[...], wg_ref[slot, :, cols], preferred_element_type=jnp.float32)
                v = jnp.dot(xg[...], wu_ref[slot, :, cols], preferred_element_type=jnp.float32)
                hid[:, cols] = (jax.nn.silu(u) * v).astype(jnp.bfloat16)

            @pl.when(b == 0)
            def _():
                now[2].wait()

            @pl.when((b == n_blocks - 1) & (e + n_slots < n_local))
            def _():
                ahead[0].start()
                ahead[1].start()

            for q in range(d_model // TILE):
                o = jnp.dot(hid[...], wd_ref[slot, :, q * TILE:(q + 1) * TILE], preferred_element_type=jnp.float32)
                for k in range(TILE // LANES):
                    xs[pl.ds((q * (TILE // LANES) + k) * stride, row_block), :] = o[:, k * LANES:(k + 1) * LANES]

            def scatter(q, c):
                scatter_rows(list_ref, at, gate_ref, e * n_pad, q * STEP, xs, acc, stride)
                return c

            lax.fori_loop(0, steps, scatter, 0)
            return c

        lax.fori_loop(0, n_blocks, block, 0)

        @pl.when(e + n_slots < n_local)
        def _():
            ahead[2].start()

        return carry

    lax.fori_loop(0, n_local, expert, 0)
    out_copies = [pltpu.make_async_copy(acc.at[pl.ds(at, ref.shape[0])], ref, out_sem.at[k]) for k, (ref, at) in enumerate(zip(outs, out_places))]
    for copy in out_copies:
        copy.start()
    for copy in out_copies:
        copy.wait()


def solution(mesh):
    n_grp = mesh.shape["grp"]
    n_loc = mesh.shape["loc"]
    n_dev = n_grp * n_loc
    tok_spec = P(("part", "grp", "loc"), None)
    w_spec = P(("grp", "loc"), None, None)

    def swap_grp(a, bits):
        return lax.ppermute(a, "grp", [(i, i ^ bits) for i in range(n_grp)])

    def swap_loc(a):
        return lax.ppermute(a, "loc", [(i, i ^ 1) for i in range(n_loc)])

    def swap_diag(a):
        pairs = [(l * n_grp + g, (l ^ 1) * n_grp + (g ^ 2)) for l in range(n_loc) for g in range(n_grp)]
        return lax.ppermute(a, ("loc", "grp"), pairs)

    def device_step(x_tok, expert_ids, gate_val, w_gate, w_up, w_down):
        tok_local, d_model = x_tok.shape
        d_ff = w_gate.shape[2]
        chunks = d_model // LANES
        n_local = w_gate.shape[0]
        per_group = n_local * n_loc
        n_tok = tok_local * n_dev
        top_k = expert_ids.shape[1]
        capacity = 8 * (n_tok * top_k // (4 * per_group * n_grp) + 1)
        me = lax.axis_index("grp") * n_loc + lax.axis_index("loc")

        meta = jnp.concatenate([expert_ids.astype(jnp.float32).T, gate_val.T], axis=0)
        meta_all = pl.pallas_call(
            functools.partial(share_kernel, n_grp, n_loc),
            out_shape=jax.ShapeDtypeStruct((n_dev,) + meta.shape, jnp.float32),
            in_specs=[pl.BlockSpec(memory_space=pltpu.VMEM)],
            out_specs=pl.BlockSpec(memory_space=pltpu.VMEM),
            scratch_shapes=[pltpu.SemaphoreType.DMA((n_dev,)), pltpu.SemaphoreType.DMA((n_dev,))],
            compiler_params=pltpu.CompilerParams(collective_id=0, has_side_effects=True),
            name="share",
        )(meta)
        mid = tok_local // 2
        low, high = (x_tok[h * mid:(h + 1) * mid].reshape(mid, chunks, LANES) for h in range(2))
        low, high, meta_all = lax.optimization_barrier((low, high, meta_all))

        y_low = swap_loc(low)
        c_low = swap_grp(low, 1)
        yc_low = swap_grp(y_low, 1)
        c_high = swap_grp(high, 1)
        y_high = swap_loc(high)
        x_low = swap_grp(low, 2)
        x_high = swap_grp(high, 2)
        late, x_low = lax.optimization_barrier((high, x_low))
        d_low = swap_loc(x_low)
        d_high = swap_diag(late)
        parts = {
            0: [low, high],
            1: [c_low, c_high],
            2: [x_low, x_high],
            3: [swap_grp(x_low, 1), swap_grp(x_high, 1)],
            4: [y_low, y_high],
            5: [yc_low, swap_grp(y_high, 1)],
            6: [d_low, d_high],
            7: [swap_grp(d_low, 1), swap_grp(d_high, 1)],
        }

        cube = meta_all.transpose(1, 0, 2).reshape(2 * top_k, 2, 2, 2, 2, mid)
        near = [(4, 0), (5, 0), (0, 0), (0, 1), (1, 0), (1, 1), (2, 0), (3, 0)]
        far = [(4, 1), (5, 1), (6, 0), (6, 1), (7, 0), (7, 1), (2, 1), (3, 1)]

        def join(*blocks):
            return jnp.concatenate([b.reshape(2 * top_k, -1, mid) for b in blocks], axis=1).reshape(2 * top_k, -1)

        row_block = 144
        n_rows = len(near) * mid
        n_pad = n_rows + PAD
        list_len = -(-min(capacity, n_rows) // row_block) * row_block
        both = jnp.stack([join(cube[:, 1, 0, :, 0], cube[:, 0, 0], cube[:, 0, 1, :, 0]), join(cube[:, 1, 0, :, 1], cube[:, 1, 1], cube[:, 0, 1, :, 1])])
        ids = both[:, :top_k].astype(jnp.int32)
        gates = both[:, top_k:]
        match = ids[:, None] == (jnp.arange(n_local) + me * n_local)[None, :, None, None]
        hit = jnp.any(match, axis=2)
        gate_of = jnp.sum(jnp.where(match, gates[:, None], 0.0), axis=2)
        gate_of = jnp.pad(gate_of, ((0, 0), (0, 0), (0, PAD)))
        n_blk = n_rows // LANES
        lane = jnp.arange(LANES)
        upper = (lane[:, None] <= lane[None, :]).astype(jnp.bfloat16)
        inner = jnp.dot(hit.reshape(-1, LANES).astype(jnp.bfloat16), upper, preferred_element_type=jnp.float32)
        inner = inner.reshape(2, n_local, n_blk, LANES)
        filled = inner[..., -1].astype(jnp.int32)
        blk = jnp.arange(n_blk)
        ends = jnp.sum(jnp.where(blk[:, None] >= blk[None, :], filled[:, :, None, :], 0), axis=3)
        count = ends[:, :, -1]
        place = jnp.arange(list_len)
        past = ends[:, :, None, :] <= place[:, None]
        which = jnp.sum(past.astype(jnp.int32), axis=3)
        rest = place - jnp.max(jnp.where(past, ends[:, :, None, :], 0), axis=3)
        pick = (which[..., None] == blk).astype(jnp.bfloat16)
        ranks = jnp.einsum("qepb,qebi->qepi", pick, inner.astype(jnp.bfloat16), preferred_element_type=jnp.float32)
        within = jnp.sum((ranks <= rest[..., None].astype(jnp.float32)).astype(jnp.int32), axis=3)
        rows = jnp.where(which < n_blk, which * LANES + within, n_rows + place % PAD)
        feeds = [(count[p], rows[p].reshape(-1), gate_of[p].reshape(-1)) for p in range(2)]

        any_spec = pl.BlockSpec(memory_space=pl.ANY)
        piece = jax.ShapeDtypeStruct((mid, chunks, LANES), jnp.float32)

        def run_pass(p, blocks, before=None):
            x_parts = [parts[r][h] for r, h in blocks]
            x_places = [p * mid for p in range(len(blocks))]
            out_places = x_places
            stride = row_block + 4
            count_p, rows_p, gates_p = feeds[p]
            if before is not None:
                count_p, before = lax.optimization_barrier((count_p, before))
            run = pl.pallas_call(
                functools.partial(pass_kernel, SLOTS, n_local, list_len, n_pad, row_block, x_places, out_places),
                grid_spec=pltpu.PrefetchScalarGridSpec(
                    num_scalar_prefetch=3,
                    grid=(),
                    in_specs=[any_spec] * (len(x_parts) + 3),
                    out_specs=[any_spec] * len(out_places),
                    scratch_shapes=[
                        pltpu.VMEM((n_pad, chunks, LANES), jnp.bfloat16),
                        pltpu.VMEM((n_pad, chunks, LANES), jnp.float32),
                        pltpu.VMEM((chunks * stride, LANES), jnp.float32),
                        pltpu.VMEM((row_block, d_model), jnp.bfloat16),
                        pltpu.VMEM((row_block, d_ff), jnp.bfloat16),
                        pltpu.VMEM((SLOTS, d_model, d_ff), jnp.bfloat16),
                        pltpu.VMEM((SLOTS, d_model, d_ff), jnp.bfloat16),
                        pltpu.VMEM((SLOTS, d_ff, d_model), jnp.bfloat16),
                        pltpu.SemaphoreType.DMA((len(x_parts),)),
                        pltpu.SemaphoreType.DMA((SLOTS, 3)),
                        pltpu.SemaphoreType.DMA((len(out_places),)),
                    ],
                ),
                out_shape=[piece] * len(out_places),
                compiler_params=pltpu.CompilerParams(vmem_limit_bytes=62_000_000),
                cost_estimate=pl.CostEstimate(flops=25 * 10**9, bytes_accessed=110 * 10**6, transcendentals=0),
            )
            outs = run(count_p, rows_p, gates_p, *x_parts, w_gate, w_up, w_down)
            return {**(before or {}), **dict(zip(blocks, outs))}

        pieces = run_pass(0, near)
        pieces = run_pass(1, far, pieces)

        totals = [None, None]
        for k, h in [(0, 0), (1, 0), (2, 0), (2, 1), (3, 0), (3, 1), (1, 1), (0, 1)]:
            send, keep = pieces[k + n_grp, h], pieces[k, h]
            mixed = (keep + swap_loc(send)).astype(jnp.bfloat16)
            back = (swap_grp(mixed, k) if k else mixed).astype(jnp.float32)
            totals[h] = back if totals[h] is None else totals[h] + back
        y = jnp.concatenate(totals, axis=0).astype(jnp.bfloat16)
        return y.reshape(tok_local, d_model)

    return jax.shard_map(device_step, mesh=mesh, in_specs=(tok_spec, tok_spec, tok_spec, w_spec, w_spec, w_spec), out_specs=tok_spec, check_vma=False)
```

```python
import functools

import jax
import jax.numpy as jnp
from jax import lax
from jax.experimental import pallas as pl
from jax.experimental.pallas import tpu as pltpu
from jax.sharding import PartitionSpec as P


MESH = pl.DeviceIdType.MESH
LANES = 128
TILE = 256
PAD = 16
STEP = 16
SLOTS = 3


def share_kernel(n_grp, n_loc, ids_ref, gate_ref, all_ref, mine_ref, send_sem, recv_sem):
    grp, loc = lax.axis_index("grp"), lax.axis_index("loc")
    n_dev = n_grp * n_loc

    def peer(r):
        return {"grp": grp ^ (r % n_grp), "loc": loc ^ (r // n_grp)}

    top_k = ids_ref.shape[0]
    mine_ref[:top_k, :] = ids_ref[...].astype(jnp.float32)
    mine_ref[top_k:, :] = gate_ref[...]
    barrier = pltpu.get_barrier_semaphore()
    for r in range(1, n_dev):
        pl.semaphore_signal(barrier, inc=1, device_id=peer(r), device_id_type=MESH)
    pl.semaphore_wait(barrier, n_dev - 1)
    copies = []
    for r in range(1, n_dev):
        copy = pltpu.make_async_remote_copy(
            src_ref=mine_ref, dst_ref=all_ref.at[r], send_sem=send_sem.at[r], recv_sem=recv_sem.at[r], device_id=peer(r), device_id_type=MESH
        )
        copy.start()
        copies.append(copy)
    all_ref[0] = mine_ref[...]
    for copy in copies:
        copy.wait()


def zero_acc(acc):
    def zero(i, c):
        acc[pl.ds(i * 16, 16)] = jnp.zeros((16,) + acc.shape[1:], jnp.float32)
        return c

    lax.fori_loop(0, acc.shape[0] // 16, zero, 0)


def gather_rows(list_ref, at, first, x_ref, xs, stride):
    chunks = x_ref.shape[1]
    for k in range(STEP):
        row = x_ref[list_ref[at + (first + k)]]
        xs[pl.ds(first + k, chunks, stride=stride), :] = row.astype(jnp.float32)


def scatter_rows(list_ref, at, gate_ref, gate_at, first, ot, acc, stride):
    chunks = acc.shape[1]
    for k0 in range(0, STEP, 4):
        slots, sums = [], []
        for k in range(k0, k0 + 4):
            s = list_ref[at + (first + k)]
            slots.append(s)
            sums.append(acc[s] + gate_ref[gate_at + s] * ot[pl.ds(first + k, chunks, stride=stride), :])
        for s, v in zip(slots, sums):
            acc[s] = v


def pass_kernel(n_slots, n_local, list_len, n_pad, row_block, x_places, out_places, cnt_ref, list_ref, gate_ref, *refs):
    n_x, n_out = len(x_places), len(out_places)
    stride = row_block + 4
    x_hbm, (wg_hbm, wu_hbm, wd_hbm), refs = refs[:n_x], refs[n_x:n_x + 3], refs[n_x + 3:]
    outs, (x_ref, acc, xs, xg, hid, wg_ref, wu_ref, wd_ref, x_sem, w_sem, out_sem) = refs[:n_out], refs[n_out:]
    d_ff, d_model = wd_ref.shape[1:]

    def weights(e, slot):
        return [
            pltpu.make_async_copy(wg_hbm.at[e], wg_ref.at[slot], w_sem.at[slot, 0]),
            pltpu.make_async_copy(wu_hbm.at[e], wu_ref.at[slot], w_sem.at[slot, 1]),
            pltpu.make_async_copy(wd_hbm.at[e], wd_ref.at[slot], w_sem.at[slot, 2]),
        ]

    x_copies = [pltpu.make_async_copy(src, x_ref.at[pl.ds(at, src.shape[0])], x_sem.at[k]) for k, (src, at) in enumerate(zip(x_hbm, x_places))]
    for copy in x_copies:
        copy.start()
    for e in range(n_slots):
        for copy in weights(e, e):
            copy.start()
    zero_acc(acc)
    for copy in x_copies:
        copy.wait()

    def expert(e, carry):
        slot = lax.rem(e, n_slots)
        n = cnt_ref[e]
        now = weights(e, slot)
        ahead = weights(e + n_slots, slot)
        n_blocks = jnp.maximum((n + row_block - 1) // row_block, 1)

        def block(b, c):
            base = b * row_block
            at = e * list_len + base
            steps = (jnp.minimum(row_block, n - base) + STEP - 1) // STEP

            def gather(q, c):
                gather_rows(list_ref, at, q * STEP, x_ref, xs, stride)
                return c

            lax.fori_loop(0, steps, gather, 0)
            for j in range(d_model // LANES):
                xg[:, j * LANES:(j + 1) * LANES] = xs[pl.ds(j * stride, row_block), :].astype(jnp.bfloat16)

            @pl.when(b == 0)
            def _():
                now[0].wait()
                now[1].wait()

            for q in range(d_ff // TILE):
                cols = slice(q * TILE, (q + 1) * TILE)
                u = jnp.dot(xg[...], wg_ref[slot, :, cols], preferred_element_type=jnp.float32)
                v = jnp.dot(xg[...], wu_ref[slot, :, cols], preferred_element_type=jnp.float32)
                hid[:, cols] = (jax.nn.silu(u) * v).astype(jnp.bfloat16)

            @pl.when(b == 0)
            def _():
                now[2].wait()

            @pl.when((b == n_blocks - 1) & (e + n_slots < n_local))
            def _():
                ahead[0].start()
                ahead[1].start()

            for q in range(d_model // TILE):
                o = jnp.dot(hid[...], wd_ref[slot, :, q * TILE:(q + 1) * TILE], preferred_element_type=jnp.float32)
                for k in range(TILE // LANES):
                    xs[pl.ds((q * (TILE // LANES) + k) * stride, row_block), :] = o[:, k * LANES:(k + 1) * LANES]

            def scatter(q, c):
                scatter_rows(list_ref, at, gate_ref, e * n_pad, q * STEP, xs, acc, stride)
                return c

            lax.fori_loop(0, steps, scatter, 0)
            return c

        lax.fori_loop(0, n_blocks, block, 0)

        @pl.when(e + n_slots < n_local)
        def _():
            ahead[2].start()

        return carry

    lax.fori_loop(0, n_local, expert, 0)
    out_copies = [pltpu.make_async_copy(acc.at[pl.ds(at, ref.shape[0])], ref, out_sem.at[k]) for k, (ref, at) in enumerate(zip(outs, out_places))]
    for copy in out_copies:
        copy.start()
    for copy in out_copies:
        copy.wait()


def solution(mesh):
    n_grp = mesh.shape["grp"]
    n_loc = mesh.shape["loc"]
    n_dev = n_grp * n_loc
    tok_spec = P(("part", "grp", "loc"), None)
    w_spec = P(("grp", "loc"), None, None)

    def swap_grp(a, bits):
        return lax.ppermute(a, "grp", [(i, i ^ bits) for i in range(n_grp)])

    def swap_loc(a):
        return lax.ppermute(a, "loc", [(i, i ^ 1) for i in range(n_loc)])

    def swap_diag(a):
        pairs = [(l * n_grp + g, (l ^ 1) * n_grp + (g ^ 2)) for l in range(n_loc) for g in range(n_grp)]
        return lax.ppermute(a, ("loc", "grp"), pairs)

    def device_step(x_tok, expert_ids, gate_val, w_gate, w_up, w_down):
        tok_local, d_model = x_tok.shape
        d_ff = w_gate.shape[2]
        chunks = d_model // LANES
        n_local = w_gate.shape[0]
        per_group = n_local * n_loc
        n_tok = tok_local * n_dev
        top_k = expert_ids.shape[1]
        capacity = 8 * (n_tok * top_k // (4 * per_group * n_grp) + 1)
        me = lax.axis_index("grp") * n_loc + lax.axis_index("loc")

        meta_all = pl.pallas_call(
            functools.partial(share_kernel, n_grp, n_loc),
            out_shape=jax.ShapeDtypeStruct((n_dev, 2 * top_k, tok_local), jnp.float32),
            in_specs=[pl.BlockSpec(memory_space=pltpu.VMEM)] * 2,
            out_specs=pl.BlockSpec(memory_space=pltpu.VMEM),
            scratch_shapes=[pltpu.VMEM((2 * top_k, tok_local), jnp.float32), pltpu.SemaphoreType.DMA((n_dev,)), pltpu.SemaphoreType.DMA((n_dev,))],
            compiler_params=pltpu.CompilerParams(collective_id=0, has_side_effects=True),
            name="share",
        )(expert_ids.T, gate_val.T)
        mid = tok_local // 2
        low, high = (x_tok[h * mid:(h + 1) * mid].reshape(mid, chunks, LANES) for h in range(2))
        low, high, meta_all = lax.optimization_barrier((low, high, meta_all))

        y_low = swap_loc(low)
        c_low = swap_grp(low, 1)
        yc_low = swap_grp(y_low, 1)
        c_high = swap_grp(high, 1)
        y_high = swap_loc(high)
        x_low = swap_grp(low, 2)
        x_high = swap_grp(high, 2)
        late, x_low = lax.optimization_barrier((high, x_low))
        d_low = swap_loc(x_low)
        d_high = swap_diag(late)
        parts = {
            0: [low, high],
            1: [c_low, c_high],
            2: [x_low, x_high],
            3: [swap_grp(x_low, 1), swap_grp(x_high, 1)],
            4: [y_low, y_high],
            5: [yc_low, swap_grp(y_high, 1)],
            6: [d_low, d_high],
            7: [swap_grp(d_low, 1), swap_grp(d_high, 1)],
        }

        cube = meta_all.transpose(1, 0, 2).reshape(2 * top_k, 2, 2, 2, 2, mid)
        near = [(4, 0), (5, 0), (0, 0), (0, 1), (1, 0), (1, 1), (2, 0), (3, 0)]
        far = [(4, 1), (5, 1), (6, 0), (6, 1), (7, 0), (7, 1), (2, 1), (3, 1)]

        def join(*blocks):
            return jnp.concatenate([b.reshape(2 * top_k, -1, mid) for b in blocks], axis=1).reshape(2 * top_k, -1)

        row_block = 144
        n_rows = len(near) * mid
        n_pad = n_rows + PAD
        list_len = -(-min(capacity, n_rows) // row_block) * row_block
        both = jnp.stack([join(cube[:, 1, 0, :, 0], cube[:, 0, 0], cube[:, 0, 1, :, 0]), join(cube[:, 1, 0, :, 1], cube[:, 1, 1], cube[:, 0, 1, :, 1])])
        ids = both[:, :top_k].astype(jnp.int32)
        gates = both[:, top_k:]
        match = ids[:, None] == (jnp.arange(n_local) + me * n_local)[None, :, None, None]
        hit = jnp.any(match, axis=2)
        gate_of = jnp.sum(jnp.where(match, gates[:, None], 0.0), axis=2)
        gate_of = jnp.pad(gate_of, ((0, 0), (0, 0), (0, PAD)))
        n_blk = n_rows // LANES
        lane = jnp.arange(LANES)
        upper = (lane[:, None] <= lane[None, :]).astype(jnp.bfloat16)
        inner = jnp.dot(hit.reshape(-1, LANES).astype(jnp.bfloat16), upper, preferred_element_type=jnp.float32)
        inner = inner.reshape(2, n_local, n_blk, LANES)
        filled = inner[..., -1].astype(jnp.int32)
        blk = jnp.arange(n_blk)
        ends = jnp.sum(jnp.where(blk[:, None] >= blk[None, :], filled[:, :, None, :], 0), axis=3)
        count = ends[:, :, -1]
        place = jnp.arange(list_len)
        past = ends[:, :, None, :] <= place[:, None]
        which = jnp.sum(past.astype(jnp.int32), axis=3)
        rest = place - jnp.max(jnp.where(past, ends[:, :, None, :], 0), axis=3)
        pick = (which[..., None] == blk).astype(jnp.bfloat16)
        ranks = jnp.einsum("qepb,qebi->qepi", pick, inner.astype(jnp.bfloat16), preferred_element_type=jnp.float32)
        within = jnp.sum((ranks <= rest[..., None].astype(jnp.float32)).astype(jnp.int32), axis=3)
        rows = jnp.where(which < n_blk, which * LANES + within, n_rows + place % PAD)
        feeds = [(count[p], rows[p].reshape(-1), gate_of[p].reshape(-1)) for p in range(2)]

        any_spec = pl.BlockSpec(memory_space=pl.ANY)
        piece = jax.ShapeDtypeStruct((mid, chunks, LANES), jnp.float32)

        def run_pass(p, blocks, before=None):
            x_parts = [parts[r][h] for r, h in blocks]
            x_places = [p * mid for p in range(len(blocks))]
            out_places = x_places
            stride = row_block + 4
            count_p, rows_p, gates_p = feeds[p]
            if before is not None:
                count_p, before = lax.optimization_barrier((count_p, before))
            run = pl.pallas_call(
                functools.partial(pass_kernel, SLOTS, n_local, list_len, n_pad, row_block, x_places, out_places),
                grid_spec=pltpu.PrefetchScalarGridSpec(
                    num_scalar_prefetch=3,
                    grid=(),
                    in_specs=[any_spec] * (len(x_parts) + 3),
                    out_specs=[any_spec] * len(out_places),
                    scratch_shapes=[
                        pltpu.VMEM((n_pad, chunks, LANES), jnp.bfloat16),
                        pltpu.VMEM((n_pad, chunks, LANES), jnp.float32),
                        pltpu.VMEM((chunks * stride, LANES), jnp.float32),
                        pltpu.VMEM((row_block, d_model), jnp.bfloat16),
                        pltpu.VMEM((row_block, d_ff), jnp.bfloat16),
                        pltpu.VMEM((SLOTS, d_model, d_ff), jnp.bfloat16),
                        pltpu.VMEM((SLOTS, d_model, d_ff), jnp.bfloat16),
                        pltpu.VMEM((SLOTS, d_ff, d_model), jnp.bfloat16),
                        pltpu.SemaphoreType.DMA((len(x_parts),)),
                        pltpu.SemaphoreType.DMA((SLOTS, 3)),
                        pltpu.SemaphoreType.DMA((len(out_places),)),
                    ],
                ),
                out_shape=[piece] * len(out_places),
                compiler_params=pltpu.CompilerParams(vmem_limit_bytes=62_000_000),
                cost_estimate=pl.CostEstimate(flops=25 * 10**9, bytes_accessed=110 * 10**6, transcendentals=0),
            )
            outs = run(count_p, rows_p, gates_p, *x_parts, w_gate, w_up, w_down)
            return {**(before or {}), **dict(zip(blocks, outs))}

        pieces = run_pass(0, near)
        pieces = run_pass(1, far, pieces)

        totals = [None, None]
        for k, h in [(0, 0), (1, 0), (2, 0), (2, 1), (3, 0), (3, 1), (1, 1), (0, 1)]:
            send, keep = pieces[k + n_grp, h], pieces[k, h]
            mixed = (keep + swap_loc(send)).astype(jnp.bfloat16)
            back = (swap_grp(mixed, k) if k else mixed).astype(jnp.float32)
            totals[h] = back if totals[h] is None else totals[h] + back
        y = jnp.concatenate(totals, axis=0).astype(jnp.bfloat16)
        return y.reshape(tok_local, d_model)

    return jax.shard_map(device_step, mesh=mesh, in_specs=(tok_spec, tok_spec, tok_spec, w_spec, w_spec, w_spec), out_specs=tok_spec, check_vma=False)
```
